32 devices in a mesh: lat: 4 (over z), lon: 4 (over y, x), fold: 2 (over core).
Axes of the slice: x: 2, y: 2, z: 4, core: 2. Of those that a mesh axis runs over, the one named last changes fastest.
Arguments:
- field: float32 [2, 12, 640, 2560], P('fold', None, 'lat', 'lon'), may hold values from -6 to 6
- row_shift: int32 [2, 12, 640, 2560], P('fold', None, 'lat', 'lon'), may hold values from -4 to 4
- col_shift: int32 [2, 12, 640, 2560], P('fold', None, 'lat', 'lon'), may hold values from -4 to 4
- row_frac: bfloat16 [2, 12, 640, 2560], P('fold', None, 'lat', 'lon'), may hold values from 0 to 1
- col_frac: bfloat16 [2, 12, 640, 2560], P('fold', None, 'lat', 'lon'), may hold values from 0 to 1
- wave_map: int32 [16], replicated, may hold values from 0 to 1279, as said below
- legendre: float32 [16, 640, 1280], P('lon', 'lat'), may hold values from -0.25 to 0.25
- helm_coef: float32 [12], P('fold'), may hold values from 1e-06 to 0.0001
Outputs:
- spectrum: float32 [12, 4, 4, 2560], P('fold', 'lon', 'lat')
The draws below stay inside these ranges and needn't reach their ends.
Inputs may be any that keep to these rules, and one draw needn't show every extreme that they name: `col_shift`: longitude offset of the departure cell. `wave_map`: distinct zonal wavenumbers.
All inputs are finite; a program needn't handle non-finite values.
Results may differ from the reference program's by a relative error of at most 0.0003.
Values sent between devices are 32-bit elements; how exact they have to be, the bound alone decides.
A program may use at most 64 MiB of HBM per device.

```python
import math
import jax
import jax.numpy as jnp
from jax import lax

LAT_HALF = 640
LON_CELLS = 2560
DEGREES = 1280
SHIFT_MAX = 4
LEVEL_DEV = 12
GROUPS = 2
LEVELS = 12
WAVES_LON = 4
WAVE_SLOTS = 16
N_LON = 4


def draw_wave_map(key, part):
    ordering = jax.random.permutation(key, DEGREES)
    return ordering[:WAVE_SLOTS].astype(jnp.int32)


def plant(result, key, least, largest):
    shape = result.shape
    index_at = [jax.random.randint(jax.random.fold_in(key, axis), (), 0, shape[axis]) for axis in range(len(shape))]
    result = result.at[tuple(index_at)].set(least)
    longest = shape.index(max(shape))
    index_at[longest] = (index_at[longest] + 1) % shape[longest]
    return result.at[tuple(index_at)].set(largest)


def level_of(key, extent, split, smallest, top_value):
    def one(dim, blocks):
        steps = jax.random.uniform(jax.random.fold_in(jax.random.fold_in(key, 6), dim), (blocks,), jnp.float32, smallest / len(split), top_value / len(split))
        return jnp.repeat(jnp.exp(steps), extent[dim] // blocks).reshape((-1,) + (1,) * (len(extent) - dim - 1))

    level = one(*split[0])
    for cut in split[1:]:
        level = level * one(*cut)
    return level


def gaussian(stream_key, dims, scale, bound, pieces=(), held_as=jnp.bfloat16):
    factor_of = level_of(stream_key, dims, pieces, -0.22, 0.18) if pieces else 1.0
    drawn = jax.random.normal(stream_key, dims, jnp.float32) * scale * factor_of
    return jnp.minimum(jnp.maximum(drawn, -bound), bound).astype(held_as)


def setup_inputs(seed: int = 0) -> dict:
    seeds = jax.random.split(jax.random.key(seed), 9)
    return {
        "field": gaussian(seeds[0], (GROUPS, LEVEL_DEV, LAT_HALF, LON_CELLS), 1.0, 6.0, ((0, 2), (2, 4), (3, 4)), jnp.float32),
        "row_shift": plant(jax.random.randint(seeds[1], (GROUPS, LEVEL_DEV, LAT_HALF, LON_CELLS), 0 - SHIFT_MAX, SHIFT_MAX + 1), jax.random.fold_in(seeds[1], 1), 0 - SHIFT_MAX, SHIFT_MAX).astype(jnp.int32),
        "col_shift": plant(jax.random.randint(seeds[2], (GROUPS, LEVEL_DEV, LAT_HALF, LON_CELLS), 0 - SHIFT_MAX, SHIFT_MAX + 1), jax.random.fold_in(seeds[2], 1), 0 - SHIFT_MAX, SHIFT_MAX).astype(jnp.int32),
        "row_frac": jnp.clip(1.0 * jax.random.uniform(seeds[3], (GROUPS, LEVEL_DEV, LAT_HALF, LON_CELLS), jnp.float32) ** level_of(seeds[3], (GROUPS, LEVEL_DEV, LAT_HALF, LON_CELLS), ((0, 2), (2, 4), (3, 4)), -0.2, 0.2), 0.0, 1.0).astype(jnp.bfloat16),
        "col_frac": jnp.clip(1.0 * jax.random.uniform(seeds[4], (GROUPS, LEVEL_DEV, LAT_HALF, LON_CELLS), jnp.float32) ** level_of(seeds[4], (GROUPS, LEVEL_DEV, LAT_HALF, LON_CELLS), ((0, 2), (2, 4), (3, 4)), -0.2, 0.2), 0.0, 1.0).astype(jnp.bfloat16),
        "wave_map": draw_wave_map(jax.random.fold_in(seeds[8], 71), 0),
        "legendre": gaussian(seeds[6], (WAVE_SLOTS, LAT_HALF, DEGREES), LAT_HALF ** -0.5, 0.25, ((0, 4), (1, 4)), jnp.float32),
        "helm_coef": jnp.clip(jnp.exp(math.log(0.0001) - 4.6051702 * jax.random.uniform(seeds[7], (LEVELS,), jnp.float32) ** level_of(seeds[7], (LEVELS,), ((0, 2),), -0.2, 0.2)), 9.999999974752427e-07, 0.0001),
    }


def cubic_weights(fraction):
    return (-fraction * (fraction - 1.0) * (fraction - 2.0) / 6.0, (fraction + 1.0) * (fraction - 1.0) * (fraction - 2.0) / 2.0, -(fraction + 1.0) * fraction * (fraction - 2.0) / 2.0, (fraction + 1.0) * fraction * (fraction - 1.0) / 6.0)

def interpolate(padded, row_shift, col_shift, row_frac, col_frac, margin):
    levels, rows, cols = row_shift.shape
    width = cols + 2 * margin
    flat = padded.reshape(levels, -1)
    row_base = lax.broadcasted_iota(jnp.int32, (levels, rows, cols), 1) + row_shift + (margin - 1)
    col_base = lax.broadcasted_iota(jnp.int32, (levels, rows, cols), 2) + col_shift + (margin - 1)
    start_index = (row_base * width + col_base).reshape(levels, -1).astype(jnp.int32)
    row_weights = cubic_weights(row_frac.astype(jnp.float32).reshape(levels, -1))
    col_weights = cubic_weights(col_frac.astype(jnp.float32).reshape(levels, -1))
    total = jnp.zeros(start_index.shape, jnp.float32)
    for row_step in range(4):
        line = jnp.zeros(start_index.shape, jnp.float32)
        for col_step in range(4):
            taken = jnp.take_along_axis(flat, start_index + (row_step * width + col_step), axis=1)
            line = line + col_weights[col_step] * taken
        total = total + row_weights[row_step] * line
    return total.reshape(levels, rows, cols)

def zonal_table(waves, first_col, count_cols, lon_total):
    col_ids = first_col + lax.iota(jnp.int32, count_cols)
    phase = col_ids[:, None] * waves[None, :] % lon_total
    angle = phase.astype(jnp.float32) * (2.0 * math.pi / lon_total)
    return jnp.stack([jnp.cos(angle), -jnp.sin(angle)], axis=1) / math.sqrt(lon_total)

def reference(field, row_shift, col_shift, row_frac, col_frac, wave_map, legendre, helm_coef):
    margin = SHIFT_MAX + 2
    blocks = GROUPS // 2
    fields = field.reshape(blocks, 2, LEVEL_DEV, LAT_HALF, LON_CELLS)
    opposite = fields[:, ::-1]
    band = opposite[:, :, :, ::-1, :][:, :, :, :margin, :]
    polar = jnp.zeros((blocks, 2, LEVEL_DEV, margin, LON_CELLS), jnp.float32)
    extended = jnp.concatenate([polar, fields, band], axis=3)
    extended = jnp.concatenate([extended[..., -margin:], extended, extended[..., :margin]], axis=4)
    number = blocks * 2 * LEVEL_DEV

    def one_field(items):
        padded, shift_rows, shift_cols, frac_rows, frac_cols = items
        return interpolate(padded[None], shift_rows[None], shift_cols[None], frac_rows[None], frac_cols[None], margin)[0]
    gridded = lax.map(one_field, (extended.reshape(number, LAT_HALF + 2 * margin, LON_CELLS + 2 * margin), row_shift.reshape(number, LAT_HALF, LON_CELLS), col_shift.reshape(number, LAT_HALF, LON_CELLS), row_frac.reshape(number, LAT_HALF, LON_CELLS), col_frac.reshape(number, LAT_HALF, LON_CELLS)))
    gridded = gridded.reshape(blocks, 2, LEVEL_DEV, LAT_HALF, LON_CELLS)
    even = (gridded[:, 0] + gridded[:, 1]).reshape(LEVELS, LAT_HALF, LON_CELLS)
    odd = (gridded[:, 0] - gridded[:, 1]).reshape(LEVELS, LAT_HALF, LON_CELLS)
    table = zonal_table(wave_map, 0, LON_CELLS, LON_CELLS)
    zonal_even = jnp.einsum('lkx,xqs->lsqk', even, table, precision=lax.Precision.HIGHEST)
    zonal_odd = jnp.einsum('lkx,xqs->lsqk', odd, table, precision=lax.Precision.HIGHEST)
    sum_even = jnp.einsum('lsqk,skn->lsqn', zonal_even, legendre, precision=lax.Precision.HIGHEST)
    sum_odd = jnp.einsum('lsqk,skn->lsqn', zonal_odd, legendre, precision=lax.Precision.HIGHEST)
    degrees = jnp.arange(DEGREES, dtype=jnp.int32)
    parity = (wave_map[:, None] + degrees[None, :]) % 2 == 0
    keep = (degrees[None, :] >= wave_map[:, None]).astype(jnp.float32)
    legendre_sum = jnp.where(parity[None, :, None, :], sum_even, sum_odd) * keep[None, :, None, :]
    degree_float = degrees.astype(jnp.float32)
    damping = 1.0 + helm_coef[:, None, None, None] * (degree_float * (degree_float + 1.0))[None, None, None, :]
    spectrum = legendre_sum / damping
    return spectrum.reshape(LEVELS, N_LON, WAVES_LON, 2 * DEGREES)
```

```python
import functools
import math

import jax
import jax.numpy as jnp
from jax import lax
from jax.experimental import pallas as pl
from jax.experimental.pallas import tpu as pltpu
from jax.sharding import PartitionSpec as P

SHIFT_MAX = 4
LANES = 128
SUBS = 8
TAPS = range(-1 - SHIFT_MAX, SHIFT_MAX + 3)
SLOTS = LANES // SUBS


def cubic_weights(t):
    tm, tp, td = t - 1.0, t + 1.0, t - 2.0
    outer = t * tm
    inner = tp * td
    return (
        outer * (td * (-1.0 / 6.0)),
        inner * (tm * 0.5),
        inner * (t * -0.5),
        outer * (tp * (1.0 / 6.0)),
    )


def gather_rows(x, index):
    dims = lax.GatherDimensionNumbers(
        offset_dims=(),
        collapsed_slice_dims=(0,),
        start_index_map=(0,),
        operand_batching_dims=(1,),
        start_indices_batching_dims=(1,),
    )
    mode = lax.GatherScatterMode.PROMISE_IN_BOUNDS
    return lax.gather(x, index[..., None], dims, (1, 1), mode=mode)


def interp_kernel(
    field,
    north,
    south,
    west,
    east,
    corners_west,
    corners_east,
    row_shift,
    col_shift,
    row_frac,
    col_frac,
    table,
    out,
    source_even,
    source_odd,
    grid,
):
    step = pl.program_id(0)
    levels = pl.num_programs(0) - 1
    rows, cols = field.shape[1:]
    count = cols // LANES
    blocks = rows // SUBS
    lane = lax.broadcasted_iota(jnp.int32, (SUBS, LANES), 1)
    sub = lax.broadcasted_iota(jnp.int32, (SUBS, LANES), 0)

    def spread(store, block, middle, left, right):
        at = pl.ds(pl.multiple_of(SUBS * block, SUBS), SUBS)
        tiles = [left, *middle, right]
        for c, move in enumerate(TAPS):
            side = (move > 0) - (move < 0)
            lowest = 1 + min(0, side)
            near = tiles[lowest : lowest + count + abs(side)]
            if side:
                near = [pltpu.roll(x, -move % LANES, 1) for x in near]
            for t in range(count):
                if side > 0:
                    moved = jnp.where(lane < LANES - move, near[t], near[t + 1])
                elif side < 0:
                    moved = jnp.where(lane >= -move, near[t + 1], near[t])
                else:
                    moved = near[t]
                store[c, t, at, :] = moved

    def tiles_of(ref, at):
        return [ref[0, at, t * LANES : (t + 1) * LANES] for t in range(count)]

    def own(store, j):
        at = pl.ds(pl.multiple_of(SUBS * j, SUBS), SUBS)
        group, place = j // SLOTS, SUBS * (j % SLOTS)
        left = pltpu.roll(west[0, group], LANES - SUBS - place, 1)
        right = pltpu.roll(east[0, group], (LANES - place) % LANES, 1)
        spread(store, j + 1, tiles_of(field, at), left, right)

    def beyond(store):
        level = jnp.minimum(step, levels - 1)
        group, place = level // SLOTS, SUBS * (level % SLOTS)
        for end, (block, ref) in enumerate(((0, north), (blocks + 1, south))):
            left = pltpu.roll(corners_west[end, group], LANES - SUBS - place, 1)
            right = pltpu.roll(corners_east[end, group], (LANES - place) % LANES, 1)
            spread(store, block, tiles_of(ref, slice(0, SUBS)), left, right)

    def interpolate(store, j, t):
        at = pl.ds(pl.multiple_of(SUBS * j, SUBS), SUBS)
        cut = slice(t * LANES, (t + 1) * LANES)
        row_t = row_frac[0, at, cut].astype(jnp.float32)
        col_t = col_frac[0, at, cut].astype(jnp.float32)
        weights = cubic_weights(row_t)
        place = sub + (row_shift[0, at, cut] + SHIFT_MAX)
        low = place < SUBS
        index = place & (SUBS - 1)
        left = col_shift[0, at, cut] + SHIFT_MAX
        far = left >= SHIFT_MAX + 1
        near = jnp.where(far, left - SHIFT_MAX, left)

        def column(c):
            picked = []
            for a in range(4):
                base = SUBS * j + (SUBS - SHIFT_MAX - 1 + a)
                upper = gather_rows(store[c, t, pl.ds(base, SUBS), :], index)
                lower = gather_rows(store[c, t, pl.ds(base + SUBS, SUBS), :], index)
                picked.append(jnp.where(low, upper, lower))
            return picked

        def combine(picked):
            total = weights[0] * picked[0]
            for a in range(1, 4):
                total = total + weights[a] * picked[a]
            return total

        columns = {}
        lines = []
        for c in range(SHIFT_MAX + 4):
            for need in (c, c + SHIFT_MAX):
                if need not in columns:
                    columns[need] = column(need)
            both = zip(columns[c], columns[c + SHIFT_MAX])
            lines.append(combine([jnp.where(far, b, a) for a, b in both]))
        most = near >= 3
        lines = [jnp.where(most, lines[i + 2], lines[i]) for i in range(6)]
        near = jnp.where(most, near - 2, near)
        lines = [jnp.where(near >= 2, lines[i + 1], lines[i]) for i in range(5)]
        lines = [jnp.where(near >= 1, lines[i + 1], lines[i]) for i in range(4)]
        slopes = [lines[i + 1] - lines[i] for i in range(3)]
        bend = slopes[1] - slopes[0]
        twist = slopes[2] - slopes[1] - bend
        inner = bend + (col_t * (1.0 / 3.0) + (1.0 / 3.0)) * twist
        grid[at, cut] = lines[1] + col_t * (slopes[1] + (col_t * 0.5 - 0.5) * inner)

    def transform():
        half = table.shape[1] // 2
        values = grid[...]
        top = values.astype(jnp.bfloat16)
        rest = (values - top.astype(jnp.float32)).astype(jnp.bfloat16)
        both = jnp.dot(top, table[...], preferred_element_type=jnp.float32)
        more = jnp.dot(rest, table[:, :half], preferred_element_type=jnp.float32)
        sums = both[:, :half] + both[:, half:] + more
        out[0] = sums.T.reshape(out.shape[1:])

    def run(read, write):
        def body(j, carry):
            own(write, j)
            for t in range(count):
                interpolate(read, j, t)
            return carry

        lax.fori_loop(0, blocks, body, 0)
        beyond(write)
        transform()

    @pl.when(step == 0)
    def _():
        def first(j, carry):
            own(source_even, j)
            return carry

        lax.fori_loop(0, blocks, first, 0)
        beyond(source_even)

    @pl.when((step > 0) & (step % 2 == 1))
    def _():
        run(source_even, source_odd)

    @pl.when((step > 0) & (step % 2 == 0))
    def _():
        run(source_odd, source_even)


def interpolated_waves(field, halos, shifts, fracs, table, n_lon):
    levels, rows, cols = field.shape
    count = cols // LANES

    def per_level(x, level):
        tail = (0,) * (x.ndim - 1)
        return pl.BlockSpec((1,) + x.shape[1:], lambda i: (level(i),) + tail)

    def ahead(x):
        return per_level(x, lambda i: jnp.minimum(i, levels - 1))

    def behind(x):
        return per_level(x, lambda i: jnp.maximum(i - 1, 0))

    def whole(x):
        return pl.BlockSpec(x.shape, lambda i: (0,) * x.ndim)

    north, south, west, east, corners_west, corners_east = halos
    shape = (levels, n_lon, table.shape[1] // 2 // n_lon, rows)
    store = pltpu.VMEM((len(TAPS), count, rows + 2 * SUBS, LANES), jnp.float32)
    return pl.pallas_call(
        interp_kernel,
        grid=(levels + 1,),
        in_specs=[ahead(x) for x in (field, north, south, west, east)]
        + [whole(corners_west), whole(corners_east)]
        + [behind(x) for x in (*shifts, *fracs)]
        + [whole(table)],
        out_specs=pl.BlockSpec((1,) + shape[1:], lambda i: (jnp.maximum(i - 1, 0), 0, 0, 0)),
        out_shape=jax.ShapeDtypeStruct(shape, jnp.float32),
        scratch_shapes=[store, store, pltpu.VMEM((rows, cols), jnp.float32)],
    )(field, north, south, west, east, corners_west, corners_east, *shifts, *fracs, table)


def packed(strip):
    levels, span = strip.shape[:2]
    rows = span - 2 * SUBS

    def lanes_of(pieces):
        front, number = pieces.shape[0], pieces.shape[1]
        groups = -(-number // SLOTS)
        pieces = jnp.pad(pieces, ((0, 0), (0, groups * SLOTS - number), (0, 0), (0, 0)))
        pieces = pieces.reshape(front, groups, SLOTS, SUBS, SUBS)
        return jnp.transpose(pieces, (0, 1, 3, 2, 4)).reshape(front, groups, SUBS, LANES)

    own = lanes_of(strip[:, SUBS:-SUBS].reshape(levels, rows // SUBS, SUBS, SUBS))
    return own, lanes_of(jnp.stack([strip[:, :SUBS], strip[:, -SUBS:]]))


def zonal_table(waves, first_col, cols, lon_total):
    col = first_col + lax.iota(jnp.int32, cols)
    phase = waves[:, None] * col[None, :] % lon_total
    angle = phase.astype(jnp.float32) * (2.0 * math.pi / lon_total)
    pair = jnp.stack([jnp.cos(angle), -jnp.sin(angle)], axis=1) / math.sqrt(lon_total)
    full = pair.reshape(-1, cols)
    top = full.astype(jnp.bfloat16)
    rest = (full - lax.reduce_precision(full, 8, 7)).astype(jnp.bfloat16)
    return jnp.concatenate([top, rest], axis=0).T


def halos_of(grid):
    rows, cols = grid.shape[1:]
    n_lat, n_fold, n_lon = (lax.axis_size(a) for a in ("lat", "fold", "lon"))
    last = n_lat - 1
    at_last = lax.axis_index("lat") == last
    head, tail = grid[:, :SUBS], grid[:, rows - SUBS :]
    north = lax.ppermute(tail, "lat", [(i, i + 1) for i in range(last)])
    below = lax.ppermute(head, "lat", [(i + 1, i) for i in range(last)])
    route = [(last * n_fold + f, last * n_fold + (f ^ 1)) for f in range(n_fold)]
    mirror = lax.ppermute(tail, ("lat", "fold"), route)

    south = jnp.where(at_last, mirror[:, ::-1], below)

    def edge(a, b):
        strip = jnp.concatenate([north[:, :, a:b], grid[:, :, a:b], south[:, :, a:b]], axis=1)
        return jnp.swapaxes(strip, 1, 2)

    ring = [(i, (i + 1) % n_lon) for i in range(n_lon)]
    west = lax.ppermute(edge(cols - SUBS, cols), "lon", ring)
    east = lax.ppermute(edge(0, SUBS), "lon", [(b, a) for a, b in ring])
    west, corners_west = packed(jnp.swapaxes(west, 1, 2))
    east, corners_east = packed(jnp.swapaxes(east, 1, 2))
    return north, south, west, east, corners_west, corners_east


def scatter_sum(pieces, axis):
    count = lax.axis_size(axis)
    place = lax.axis_index(axis)
    total = lax.dynamic_index_in_dim(pieces, place, 0, keepdims=False)
    arrived = []
    for step in range(1, count):
        piece = lax.dynamic_index_in_dim(pieces, (place + step) % count, 0, keepdims=False)
        arrived.append(lax.ppermute(piece, axis, [(i, (i + step) % count) for i in range(count)]))
    for part in arrived:
        total = total + part
    return total


def local(field, row_shift, col_shift, row_frac, col_frac, wave_map, legendre, helm_coef):
    grid = field[0]
    levels, rows, cols = grid.shape
    half = levels // 2
    n_lon, n_lat, n_fold = (lax.axis_size(a) for a in ("lon", "lat", "fold"))
    lon_place = lax.axis_index("lon")
    table = zonal_table(wave_map, lon_place * cols, cols, cols * n_lon)
    halos = halos_of(grid)
    waves_here = interpolated_waves(
        grid,
        halos,
        (row_shift[0], col_shift[0]),
        (row_frac[0], col_frac[0]),
        table,
        n_lon,
    )
    slots_here = wave_map.shape[0] // n_lon
    hemisphere = lax.axis_index("fold") % 2
    sign = (1 - 2 * hemisphere).astype(jnp.float32)
    coeffs = scatter_sum(jnp.swapaxes(waves_here, 0, 1), "lon")
    outgoing = lax.dynamic_slice_in_dim(coeffs, (1 - hemisphere) * half, half, 0)
    incoming = lax.ppermute(outgoing, "fold", [(f, f ^ 1) for f in range(n_fold)])
    kept = lax.dynamic_slice_in_dim(coeffs, hemisphere * half, half, 0)
    folded = jnp.stack([kept + incoming, sign * (kept - incoming)], axis=0)
    folded = jnp.transpose(folded.reshape(2, half, slots_here, 2, rows), (2, 3, 0, 1, 4))
    degree_count = legendre.shape[2]
    degrees = lax.iota(jnp.int32, degree_count)
    waves = lax.dynamic_slice_in_dim(wave_map, lon_place * slots_here, slots_here)
    product = jnp.einsum("sqelk,skn->selqn", folded, legendre, precision=lax.Precision.HIGHEST)
    parity = (waves[:, None] + degrees[None, :]) % 2 == 0
    keep = degrees[None, :] >= waves[:, None]
    picked = jnp.where(parity[:, None, None, :], product[:, 0], product[:, 1])
    picked = jnp.where(keep[:, None, None, :], picked, 0.0)
    summed = scatter_sum(
        picked.reshape(n_lat, slots_here // n_lat, half, 2 * degree_count), "lat"
    )
    degree_float = degrees.astype(jnp.float32)
    pair = jnp.concatenate([degree_float, degree_float])
    damping = 1.0 + helm_coef[None, :, None] * (pair * (pair + 1.0))[None, None, :]
    return jnp.transpose(summed / damping, (1, 0, 2))[:, None, :, :]


def solution(mesh):
    block = P("fold", None, "lat", "lon")
    in_specs = (block,) * 5 + (P(), P("lon", "lat", None), P("fold"))
    out_specs = P("fold", "lon", "lat", None)
    return jax.shard_map(local, mesh=mesh, in_specs=in_specs, out_specs=out_specs, check_vma=False)
```

```python
import functools
import math

import jax
import jax.numpy as jnp
from jax import lax
from jax.experimental import pallas as pl
from jax.experimental.pallas import tpu as pltpu
from jax.sharding import PartitionSpec as P

SHIFT_MAX = 4
LANES = 128
SUBS = 8
TAPS = range(-1 - SHIFT_MAX, SHIFT_MAX + 3)
SLOTS = LANES // SUBS


def cubic_weights(t):
    tm, tp, td = t - 1.0, t + 1.0, t - 2.0
    outer = t * tm
    inner = tp * td
    return (
        outer * (td * (-1.0 / 6.0)),
        inner * (tm * 0.5),
        inner * (t * -0.5),
        outer * (tp * (1.0 / 6.0)),
    )


def gather_rows(x, index):
    dims = lax.GatherDimensionNumbers(
        offset_dims=(),
        collapsed_slice_dims=(0,),
        start_index_map=(0,),
        operand_batching_dims=(1,),
        start_indices_batching_dims=(1,),
    )
    mode = lax.GatherScatterMode.PROMISE_IN_BOUNDS
    return lax.gather(x, index[..., None], dims, (1, 1), mode=mode)


def interp_kernel(
    field,
    north,
    south,
    west,
    east,
    corners_west,
    corners_east,
    row_shift,
    col_shift,
    row_frac,
    col_frac,
    table,
    out,
    source_even,
    source_odd,
    grid,
):
    step = pl.program_id(0)
    levels = pl.num_programs(0) - 1
    rows, cols = field.shape[1:]
    count = cols // LANES
    blocks = rows // SUBS
    lane = lax.broadcasted_iota(jnp.int32, (SUBS, LANES), 1)
    sub = lax.broadcasted_iota(jnp.int32, (SUBS, LANES), 0)

    def spread(store, block, middle, left, right):
        at = pl.ds(pl.multiple_of(SUBS * block, SUBS), SUBS)
        tiles = [left, *middle, right]
        for c, move in enumerate(TAPS):
            side = (move > 0) - (move < 0)
            lowest = 1 + min(0, side)
            near = tiles[lowest : lowest + count + abs(side)]
            if side:
                near = [pltpu.roll(x, -move % LANES, 1) for x in near]
            for t in range(count):
                if side > 0:
                    moved = jnp.where(lane < LANES - move, near[t], near[t + 1])
                elif side < 0:
                    moved = jnp.where(lane >= -move, near[t + 1], near[t])
                else:
                    moved = near[t]
                store[c, t, at, :] = moved

    def tiles_of(ref, at):
        return [ref[0, at, t * LANES : (t + 1) * LANES] for t in range(count)]

    def own(store, j):
        at = pl.ds(pl.multiple_of(SUBS * j, SUBS), SUBS)
        group, place = j // SLOTS, SUBS * (j % SLOTS)
        left = pltpu.roll(west[0, group], LANES - SUBS - place, 1)
        right = pltpu.roll(east[0, group], (LANES - place) % LANES, 1)
        spread(store, j + 1, tiles_of(field, at), left, right)

    def beyond(store):
        level = jnp.minimum(step, levels - 1)
        group, place = level // SLOTS, SUBS * (level % SLOTS)
        for end, (block, ref) in enumerate(((0, north), (blocks + 1, south))):
            left = pltpu.roll(corners_west[end, group], LANES - SUBS - place, 1)
            right = pltpu.roll(corners_east[end, group], (LANES - place) % LANES, 1)
            spread(store, block, tiles_of(ref, slice(0, SUBS)), left, right)

    def interpolate(store, j, t):
        at = pl.ds(pl.multiple_of(SUBS * j, SUBS), SUBS)
        cut = slice(t * LANES, (t + 1) * LANES)
        row_t = row_frac[0, at, cut].astype(jnp.float32)
        col_t = col_frac[0, at, cut].astype(jnp.float32)
        weights = cubic_weights(row_t)
        place = sub + (row_shift[0, at, cut] + SHIFT_MAX)
        low = place < SUBS
        index = place & (SUBS - 1)
        left = col_shift[0, at, cut] + SHIFT_MAX
        far = left >= SHIFT_MAX + 1
        near = jnp.where(far, left - SHIFT_MAX, left)

        def column(c):
            picked = []
            for a in range(4):
                base = SUBS * j + (SUBS - SHIFT_MAX - 1 + a)
                upper = gather_rows(store[c, t, pl.ds(base, SUBS), :], index)
                lower = gather_rows(store[c, t, pl.ds(base + SUBS, SUBS), :], index)
                picked.append(jnp.where(low, upper, lower))
            return picked

        def combine(picked):
            total = weights[0] * picked[0]
            for a in range(1, 4):
                total = total + weights[a] * picked[a]
            return total

        columns = {}
        lines = []
        for c in range(SHIFT_MAX + 4):
            for need in (c, c + SHIFT_MAX):
                if need not in columns:
                    columns[need] = column(need)
            both = zip(columns[c], columns[c + SHIFT_MAX])
            lines.append(combine([jnp.where(far, b, a) for a, b in both]))
        most = near >= 3
        lines = [jnp.where(most, lines[i + 2], lines[i]) for i in range(6)]
        near = jnp.where(most, near - 2, near)
        lines = [jnp.where(near >= 2, lines[i + 1], lines[i]) for i in range(5)]
        lines = [jnp.where(near >= 1, lines[i + 1], lines[i]) for i in range(4)]
        slopes = [lines[i + 1] - lines[i] for i in range(3)]
        bend = slopes[1] - slopes[0]
        twist = slopes[2] - slopes[1] - bend
        inner = bend + (col_t * (1.0 / 3.0) + (1.0 / 3.0)) * twist
        grid[at, cut] = lines[1] + col_t * (slopes[1] + (col_t * 0.5 - 0.5) * inner)

    def transform():
        half = table.shape[1] // 2
        values = grid[...]
        top = values.astype(jnp.bfloat16)
        rest = (values - top.astype(jnp.float32)).astype(jnp.bfloat16)
        both = jnp.dot(top, table[...], preferred_element_type=jnp.float32)
        more = jnp.dot(rest, table[:, :half], preferred_element_type=jnp.float32)
        sums = both[:, :half] + both[:, half:] + more
        out[0] = sums.T.reshape(out.shape[1:])

    def run(read, write):
        def body(j, carry):
            own(write, j)
            for t in range(count):
                interpolate(read, j, t)
            return carry

        lax.fori_loop(0, blocks, body, 0)
        beyond(write)
        transform()

    @pl.when(step == 0)
    def _():
        def first(j, carry):
            own(source_even, j)
            return carry

        lax.fori_loop(0, blocks, first, 0)
        beyond(source_even)

    @pl.when((step > 0) & (step % 2 == 1))
    def _():
        run(source_even, source_odd)

    @pl.when((step > 0) & (step % 2 == 0))
    def _():
        run(source_odd, source_even)


def interpolated_waves(field, halos, shifts, fracs, table, n_lon):
    levels, rows, cols = field.shape
    count = cols // LANES

    def per_level(x, level):
        tail = (0,) * (x.ndim - 1)
        return pl.BlockSpec((1,) + x.shape[1:], lambda i: (level(i),) + tail)

    def ahead(x):
        return per_level(x, lambda i: jnp.minimum(i, levels - 1))

    def behind(x):
        return per_level(x, lambda i: jnp.maximum(i - 1, 0))

    def whole(x):
        return pl.BlockSpec(x.shape, lambda i: (0,) * x.ndim)

    north, south, west, east, corners_west, corners_east = halos
    shape = (levels, n_lon, table.shape[1] // 2 // n_lon, rows)
    store = pltpu.VMEM((len(TAPS), count, rows + 2 * SUBS, LANES), jnp.float32)
    return pl.pallas_call(
        interp_kernel,
        grid=(levels + 1,),
        in_specs=[ahead(x) for x in (field, north, south, west, east)]
        + [whole(corners_west), whole(corners_east)]
        + [behind(x) for x in (*shifts, *fracs)]
        + [whole(table)],
        out_specs=pl.BlockSpec((1,) + shape[1:], lambda i: (jnp.maximum(i - 1, 0), 0, 0, 0)),
        out_shape=jax.ShapeDtypeStruct(shape, jnp.float32),
        scratch_shapes=[store, store, pltpu.VMEM((rows, cols), jnp.float32)],
    )(field, north, south, west, east, corners_west, corners_east, *shifts, *fracs, table)


MESH = pl.DeviceIdType.MESH


def signal_to(semaphore, place):
    pl.semaphore_signal(semaphore, inc=1, device_id=place, device_id_type=MESH)


def remote(source, target, sends, receives, place):
    return pltpu.make_async_remote_copy(
        src_ref=source,
        dst_ref=target,
        send_sem=sends,
        recv_sem=receives,
        device_id=place,
        device_id_type=MESH,
    )


def halo_kernel(
    lon_total,
    field,
    wave_map,
    north,
    south,
    west,
    east,
    corners_west,
    corners_east,
    table,
    edge_west,
    edge_east,
    outside,
    to_west,
    to_east,
    corners_to_west,
    corners_to_east,
    local_sems,
    row_sends,
    north_sem,
    south_sem,
    lon_sends,
    lon_receives,
):
    levels, rows, cols = field.shape
    count = cols // LANES
    blocks = rows // SUBS
    n_lat, n_lon = lax.axis_size("lat"), lax.axis_size("lon")
    lat, lon, fold = (lax.axis_index(a) for a in ("lat", "lon", "fold"))
    last = n_lat - 1
    hemisphere = fold % 2
    partner = {"fold": fold + 1 - 2 * hemisphere}
    eastward = {"lon": lax.rem(lon + 1, n_lon)}
    westward = {"lon": lax.rem(lon + n_lon - 1, n_lon)}
    lane = lax.broadcasted_iota(jnp.int32, (SUBS, LANES), 1)
    sub = lax.broadcasted_iota(jnp.int32, (SUBS, LANES), 0)

    edges = [
        pltpu.make_async_copy(field.at[:, :, 0:LANES], edge_west, local_sems.at[0]),
        pltpu.make_async_copy(field.at[:, :, cols - LANES : cols], edge_east, local_sems.at[1]),
    ]
    for copy in edges:
        copy.start()

    barrier = pltpu.get_barrier_semaphore()
    signal_to(barrier, eastward)
    signal_to(barrier, westward)

    @pl.when(lat > 0)
    def _():
        signal_to(barrier, {"lat": lat - 1})

    @pl.when(lat < last)
    def _():
        signal_to(barrier, {"lat": lat + 1})

    @pl.when(lat == last)
    def _():
        signal_to(barrier, partner)

    pl.semaphore_wait(barrier, 3 + jnp.minimum(lat, 1))

    head = field.at[:, 0:SUBS, :]
    tail = field.at[:, rows - SUBS : rows, :]

    def southward():
        return remote(tail, north, row_sends.at[0], north_sem, {"lat": lat + 1})

    def across():
        return remote(tail, outside, row_sends.at[0], south_sem, partner)

    def northward():
        return remote(head, outside, row_sends.at[1], south_sem, {"lat": lat - 1})

    @pl.when(lat < last)
    def _():
        southward().start()

    @pl.when(lat == last)
    def _():
        across().start()

    @pl.when(lat > 0)
    def _():
        northward().start()

    for copy in edges:
        copy.wait()

    def pack_level(level, carry):
        for group in range(to_west.shape[1]):
            first = jnp.zeros((SUBS, LANES), jnp.float32)
            final = jnp.zeros((SUBS, LANES), jnp.float32)
            for k in range(min(SLOTS, blocks - group * SLOTS)):
                at = slice(SUBS * (group * SLOTS + k), SUBS * (group * SLOTS + k + 1))
                here = (lane >= SUBS * k) & (lane < SUBS * (k + 1))
                moved = edge_west[level, at, :]
                if k:
                    moved = pltpu.roll(moved, SUBS * k, 1)
                first = jnp.where(here, moved, first)
                moved = edge_east[level, at, :]
                if k < SLOTS - 1:
                    moved = pltpu.roll(moved, SUBS * (k + 1), 1)
                final = jnp.where(here, moved, final)
            to_west[level, group] = first
            to_east[level, group] = final
        return carry

    lax.fori_loop(0, levels, pack_level, 0)

    strips = [
        remote(to_west, east, lon_sends.at[0], lon_receives.at[0], westward),
        remote(to_east, west, lon_sends.at[1], lon_receives.at[1], eastward),
    ]
    for copy in strips:
        copy.start()

    width = table.shape[1] // 2
    chunk = 2 * SUBS
    column = lax.broadcasted_iota(jnp.int32, (chunk, 2 * width), 1)
    which = jnp.where(column < width, column, column - width)
    slot, part = which >> 1, which & 1
    wave = jnp.zeros((chunk, 2 * width), jnp.int32)
    for s in range(width // 2):
        wave = jnp.where(slot == s, wave_map[s], wave)
    wave = wave.astype(jnp.float32)
    quarter = part.astype(jnp.float32) * (lon_total / 4.0)
    down = lax.broadcasted_iota(jnp.int32, (chunk, 2 * width), 0)
    start = lon * cols

    def table_rows(i, carry):
        place = (start + i * chunk + down).astype(jnp.float32)
        product = wave * place
        turns = jnp.floor(product * (1.0 / lon_total))
        phase = product - turns * lon_total + quarter
        phase = jnp.where(phase < 0.0, phase + lon_total, phase)
        phase = jnp.where(phase >= lon_total, phase - lon_total, phase)
        phase = jnp.where(phase >= lon_total, phase - lon_total, phase)
        value = jnp.cos(phase * (2.0 * math.pi / lon_total)) * (1.0 / math.sqrt(lon_total))
        top = value.astype(jnp.bfloat16).astype(jnp.float32)
        both = jnp.where(column < width, top, value - top)
        table[pl.ds(pl.multiple_of(i * chunk, chunk), chunk), :] = both.astype(jnp.bfloat16)
        return carry

    lax.fori_loop(0, cols // chunk, table_rows, 0)

    @pl.when(lat > 0)
    def _():
        southward().wait_recv()

    @pl.when(lat == 0)
    def _():
        north[...] = jnp.zeros(north.shape, jnp.float32)

    across().wait_recv()
    flip = jnp.where(jnp.full((SUBS, LANES), lat, jnp.int32) == last, SUBS - 1 - sub, sub)

    corners_to_west[...] = jnp.zeros(corners_to_west.shape, jnp.float32)
    corners_to_east[...] = jnp.zeros(corners_to_east.shape, jnp.float32)

    for level in range(levels):
        for t in range(count):
            cut = slice(t * LANES, (t + 1) * LANES)
            south[level, :, cut] = gather_rows(outside[level, :, cut], flip)
    for level in range(levels):
        group, place = level // SLOTS, SUBS * (level % SLOTS)
        here = (lane >= place) & (lane < place + SUBS)
        for end, ref in enumerate((north, south)):
            moved = pltpu.roll(ref[level, :, 0:LANES], place, 1) if place else ref[level, :, 0:LANES]
            corners_to_west[end, group] = jnp.where(here, moved, corners_to_west[end, group])
            moved = ref[level, :, cols - LANES : cols]
            if place < LANES - SUBS:
                moved = pltpu.roll(moved, place + SUBS, 1)
            corners_to_east[end, group] = jnp.where(here, moved, corners_to_east[end, group])

    corners = [
        remote(corners_to_west, corners_east, lon_sends.at[2], lon_receives.at[2], westward),
        remote(corners_to_east, corners_west, lon_sends.at[3], lon_receives.at[3], eastward),
    ]
    for copy in corners:
        copy.start()
    for copy in strips + corners:
        copy.wait()
    across().wait_send()

    @pl.when(lat > 0)
    def _():
        northward().wait_send()


def exchanged_halos(field, wave_map, lon_total):
    levels, rows, cols = field.shape
    groups = -(-rows // (SUBS * SLOTS))
    vmem = pl.BlockSpec(memory_space=pltpu.VMEM)
    rows_shape = (levels, SUBS, cols)
    strip_shape = (levels, groups, SUBS, LANES)
    corner_shape = (2, -(-levels // SLOTS), SUBS, LANES)
    shapes = [rows_shape] * 2 + [strip_shape] * 2 + [corner_shape] * 2
    f32 = jnp.float32
    edge = pltpu.VMEM((levels, rows, LANES), f32)
    return pl.pallas_call(
        functools.partial(halo_kernel, lon_total),
        in_specs=[pl.BlockSpec(memory_space=pl.ANY), pl.BlockSpec(memory_space=pltpu.SMEM)],
        out_specs=[vmem] * 7,
        out_shape=[jax.ShapeDtypeStruct(s, f32) for s in shapes]
        + [jax.ShapeDtypeStruct((cols, 4 * wave_map.shape[0]), jnp.bfloat16)],
        scratch_shapes=[
            edge,
            edge,
            pltpu.VMEM(rows_shape, f32),
            pltpu.VMEM(strip_shape, f32),
            pltpu.VMEM(strip_shape, f32),
            pltpu.VMEM(corner_shape, f32),
            pltpu.VMEM(corner_shape, f32),
            pltpu.SemaphoreType.DMA((2,)),
            pltpu.SemaphoreType.DMA((2,)),
            pltpu.SemaphoreType.DMA,
            pltpu.SemaphoreType.DMA,
            pltpu.SemaphoreType.DMA((4,)),
            pltpu.SemaphoreType.DMA((4,)),
        ],
        compiler_params=pltpu.CompilerParams(collective_id=0, has_side_effects=True),
    )(field, wave_map)


def spectral_kernel(
    waves,
    legendre,
    wave_map,
    helm,
    out,
    matrix,
    matrix_top,
    matrix_rest,
    gathered,
    left,
    outgoing,
    partial,
    local_sems,
    zonal_sends,
    zonal_receives,
    lat_sends,
    lat_receives,
):
    levels, n_lon, width, rows = waves.shape
    half = levels // 2
    slots, _, degrees = legendre.shape
    n_lat = lax.axis_size("lat")
    lat, lon, fold = (lax.axis_index(a) for a in ("lat", "lon", "fold"))
    hemisphere = fold % 2
    per_lat = slots // n_lat

    load = pltpu.make_async_copy(legendre, matrix, local_sems.at[0])
    load.start()

    barrier = pltpu.get_barrier_semaphore()
    peers = [(h, p) for h in range(2) for p in range(n_lon) if h or p]

    def zonal_peer(h, p):
        other = lax.rem(hemisphere + h, 2)
        return other, {"lon": lax.rem(lon + p, n_lon), "fold": fold - hemisphere + other}

    def lat_peer(d):
        return lax.rem(lat + d, n_lat)

    for h, p in peers:
        signal_to(barrier, zonal_peer(h, p)[1])
    for d in range(1, n_lat):
        signal_to(barrier, {"lat": lat_peer(d)})

    def piece(h, p):
        level = pl.multiple_of(lax.rem(hemisphere + h, 2) * half, half)
        return waves.at[pl.ds(level, half), lax.rem(lon + p, n_lon)]

    own = pltpu.make_async_copy(piece(0, 0), gathered.at[0, 0], local_sems.at[1])
    own.start()
    pl.semaphore_wait(barrier, len(peers) + n_lat - 1)

    copies = []
    for h, p in peers:
        copy = remote(
            piece(h, p),
            gathered.at[h, p],
            zonal_sends.at[h, p],
            zonal_receives.at[h, p],
            zonal_peer(h, p)[1],
        )
        copy.start()
        copies.append(copy)

    load.wait()

    def split(s, carry):
        full = matrix[s]
        top = full.astype(jnp.bfloat16)
        matrix_top[s] = top
        matrix_rest[s] = (full - top.astype(jnp.float32)).astype(jnp.bfloat16)
        return carry

    lax.fori_loop(0, slots, split, 0)

    own.wait()
    for copy in copies:
        copy.wait()

    same = gathered[0, 0]
    other = gathered[1, 0]
    for p in range(1, n_lon):
        same = same + gathered[0, p]
        other = other + gathered[1, p]
    sign = jnp.where(jnp.full(same.shape, hemisphere, jnp.int32) == 0, 1.0, -1.0)
    for e, value in enumerate((same + other, (same - other) * sign)):
        for w in range(width):
            for level in range(half):
                at = (2 * e + w % 2) * half + level
                left[w // 2, at : at + 1, :] = value[level, w : w + 1, :]

    degree = lax.broadcasted_iota(jnp.int32, (2 * half, degrees), 1)

    def product(slot):
        full = left[slot]
        top = full.astype(jnp.bfloat16)
        rest = (full - top.astype(jnp.float32)).astype(jnp.bfloat16)
        result = jnp.dot(top, matrix_top[slot], preferred_element_type=jnp.float32)
        result = result + jnp.dot(rest, matrix_top[slot], preferred_element_type=jnp.float32)
        result = result + jnp.dot(top, matrix_rest[slot], preferred_element_type=jnp.float32)
        wave = wave_map[lon * slots + slot]
        even = ((degree + wave) & 1) == 0
        chosen = jnp.where(even, result[: 2 * half], result[2 * half :])
        return jnp.where(degree >= wave, chosen, 0.0)

    sends = []
    for d in range(n_lat - 1, 0, -1):
        place = lat_peer(d)
        for e in range(per_lat):
            outgoing[d - 1, e] = product(place * per_lat + e)
        copy = remote(
            outgoing.at[d - 1],
            partial.at[d - 1],
            lat_sends.at[d - 1],
            lat_receives.at[d - 1],
            {"lat": place},
        )
        copy.start()
        sends.append(copy)
    mine = [product(lat * per_lat + e) for e in range(per_lat)]

    scale = degree.astype(jnp.float32)
    scale = scale * (scale + 1.0)
    row = lax.broadcasted_iota(jnp.int32, (2 * half, degrees), 0)
    coefficient = jnp.zeros((2 * half, degrees), jnp.float32)
    for level in range(half):
        coefficient = jnp.where(lax.rem(row, half) == level, helm[level], coefficient)
    damping = 1.0 + coefficient * scale

    for copy in sends:
        copy.wait()
    for e in range(per_lat):
        total = mine[e]
        for d in range(n_lat - 1):
            total = total + partial[d, e]
        total = total / damping
        out[e, :, 0:degrees] = total[:half]
        out[e, :, degrees : 2 * degrees] = total[half:]


def spectral_sums(waves, legendre, wave_map, helm):
    levels, n_lon, width, rows = waves.shape
    half = levels // 2
    slots, _, degrees = legendre.shape
    n_lat = lax.axis_size("lat")
    per_lat = slots // n_lat
    f32, bf16 = jnp.float32, jnp.bfloat16
    any_space = pl.BlockSpec(memory_space=pl.ANY)
    smem = pl.BlockSpec(memory_space=pltpu.SMEM)
    moved = pltpu.VMEM((n_lat - 1, per_lat, 2 * half, degrees), f32)
    return pl.pallas_call(
        spectral_kernel,
        in_specs=[any_space, any_space, smem, smem],
        out_specs=pl.BlockSpec(memory_space=pltpu.VMEM),
        out_shape=jax.ShapeDtypeStruct((per_lat, half, 2 * degrees), f32),
        scratch_shapes=[
            pltpu.VMEM(legendre.shape, f32),
            pltpu.VMEM(legendre.shape, bf16),
            pltpu.VMEM(legendre.shape, bf16),
            pltpu.VMEM((2, n_lon, half, width, rows), f32),
            pltpu.VMEM((width // 2, 4 * half, rows), f32),
            moved,
            moved,
            pltpu.SemaphoreType.DMA((2,)),
            pltpu.SemaphoreType.DMA((2, n_lon)),
            pltpu.SemaphoreType.DMA((2, n_lon)),
            pltpu.SemaphoreType.DMA((n_lat - 1,)),
            pltpu.SemaphoreType.DMA((n_lat - 1,)),
        ],
        compiler_params=pltpu.CompilerParams(collective_id=1, has_side_effects=True),
    )(waves, legendre, wave_map, helm)


def local(field, row_shift, col_shift, row_frac, col_frac, wave_map, legendre, helm_coef):
    grid = field[0]
    n_lon = lax.axis_size("lon")
    *halos, table = exchanged_halos(grid, wave_map, grid.shape[2] * n_lon)
    waves = interpolated_waves(
        grid,
        halos,
        (row_shift[0], col_shift[0]),
        (row_frac[0], col_frac[0]),
        table,
        n_lon,
    )
    result = spectral_sums(waves, legendre, wave_map, helm_coef)
    return jnp.transpose(result, (1, 0, 2))[:, None, :, :]


def solution(mesh):
    block = P("fold", None, "lat", "lon")
    in_specs = (block,) * 5 + (P(), P("lon", "lat", None), P("fold"))
    out_specs = P("fold", "lon", "lat", None)
    return jax.shard_map(local, mesh=mesh, in_specs=in_specs, out_specs=out_specs, check_vma=False)
```
